32 devices in a mesh: gz: 8 (over z, y), gy: 4 (over x, core).
Axes of the slice: x: 2, y: 2, z: 4, core: 2. Of those that a mesh axis runs over, the one named last changes fastest.
Arguments:
- right_side: float32 [8, 16, 256, 512], P(None, 'gz', 'gy'), may hold values from -8 to 8
- diagonal: float32 [16, 256, 512], P('gz', 'gy'), may hold values from 0.1 to 4
Outputs:
- solution: float32 [8, 16, 256, 512], P(None, 'gz', 'gy')
- hessenberg: float32 [24, 32], replicated
The draws below stay inside these ranges and needn't reach their ends.
All inputs are finite; a program needn't handle non-finite values.
Results may differ from the reference program's by a relative error of at most 0.0003.
Values sent between devices are 32-bit elements; how exact they have to be, the bound alone decides.
A program may use at most 64 MiB of HBM per device.

```python
import math
import jax
import jax.numpy as jnp
from jax import lax

BLK = 8
ITERS = 3
NX = 512
NZ = 16
NY = 256


def level_of(rng, dims, shards, smallest, top_value):
    gain = 1.0
    for axis_at, shards_of in shards:
        draws = jax.random.uniform(jax.random.fold_in(jax.random.fold_in(rng, 6), axis_at), (shards_of,), jnp.float32, smallest / len(shards), top_value / len(shards))
        gain = gain * jnp.repeat(jnp.exp(draws), dims[axis_at] // shards_of).reshape((-1,) + (1,) * (len(dims) - 1 - axis_at))
    return gain


def gaussian(key, shape, deviation, most, split=(), dtype=jnp.bfloat16):
    level = level_of(key, shape, split, -0.22, 0.18) if split else 1.0
    drawn = jax.random.normal(key, shape, jnp.float32) * deviation * level
    return jnp.minimum(jnp.maximum(drawn, -most), most).astype(dtype)


def setup_inputs(seed: int = 0) -> dict:
    streams_of = jax.random.split(jax.random.key(seed), 3)
    return {
        "right_side": gaussian(streams_of[0], (BLK, NZ, NY, NX), 1.0, 8.0, ((1, 8), (2, 4)), jnp.float32),
        "diagonal": jnp.clip(jnp.exp(math.log(4.0) - 3.6888794 * jax.random.uniform(streams_of[1], (NZ, NY, NX), jnp.float32) ** level_of(streams_of[1], (NZ, NY, NX), ((0, 8), (1, 4)), -0.2, 0.2)), 0.1, 4.0),
    }


def apply_op(field, diagonal):
    padded = jnp.pad(field, ((0, 0), (1, 1), (1, 1), (1, 1)))
    beside = padded[:, 2:, 1:-1, 1:-1] + padded[:, :-2, 1:-1, 1:-1]
    beside = beside + padded[:, 1:-1, 2:, 1:-1] + padded[:, 1:-1, :-2, 1:-1]
    beside = beside + padded[:, 1:-1, 1:-1, 2:] + padded[:, 1:-1, 1:-1, :-2]
    return (6.0 + diagonal)[None] * field - beside

def inner(left, right):
    return jnp.dot(left, right.T, precision=lax.Precision.HIGHEST)

def reference(right_side, diagonal):
    shape = right_side.shape
    flat_rhs = right_side.reshape(BLK, -1)
    lower0 = jnp.linalg.cholesky(inner(flat_rhs, flat_rhs))
    basis = [jax.scipy.linalg.solve_triangular(lower0, flat_rhs, lower=True)]
    blocks = []
    for step in range(ITERS):
        work = apply_op(basis[step].reshape(shape), diagonal).reshape(BLK, -1)
        coeff = [inner(work, vec) for vec in basis]
        reduced = work
        for index in range(step + 1):
            reduced = reduced - jnp.dot(coeff[index], basis[index], precision=lax.Precision.HIGHEST)
        lower = jnp.linalg.cholesky(inner(reduced, reduced))
        basis.append(jax.scipy.linalg.solve_triangular(lower, reduced, lower=True))
        row = coeff + [lower] + [jnp.zeros((BLK, BLK), jnp.float32)] * (ITERS - 1 - step)
        blocks.append(jnp.concatenate(row, axis=1))
    hessenberg = jnp.concatenate(blocks, axis=0)
    normal = jnp.dot(hessenberg, hessenberg.T, precision=lax.Precision.HIGHEST)
    factor = jnp.linalg.cholesky(normal)
    target = jnp.dot(hessenberg[:, :BLK], lower0.T, precision=lax.Precision.HIGHEST)
    coeffs = jax.scipy.linalg.cho_solve((factor, True), target)
    stacked = jnp.concatenate(basis[:ITERS], axis=0)
    solution = jnp.dot(coeffs.T, stacked, precision=lax.Precision.HIGHEST)
    return (solution.reshape(shape), hessenberg)
```

```python
import functools

import jax
import jax.numpy as jnp
from jax import lax
from jax.experimental import pallas as pl
from jax.experimental.pallas import tpu as pltpu
from jax.sharding import PartitionSpec as P

ITERS = 3
CENTRE = 7.5
SCALE = 0.25
CHUNKS = 4
MESH = pl.DeviceIdType.MESH
HIGH = lax.Precision.HIGHEST


def nt_dot(left, right):
    return lax.dot_general(
        left, right, (((1,), (1,)), ((), ())), precision=HIGH, preferred_element_type=jnp.float32
    )


def dot(left, right):
    return jnp.dot(left, right, precision=HIGH, preferred_element_type=jnp.float32)


def kernel(
    r_ref, d_ref, out_ref, hess_ref,
    k0, k1, k2, k3, diag, ret1, ret2, ys, yh, acc, mine, slots1, part, slots2, splat,
    x_s, x_r, d_s, d_r, z_s, z_r, y_s, y_r, b_s, b_r, g1_s, g1_r, g2_s, g2_r,
):
    blk, lay, rows, nx = r_ref.shape
    half, group_lay = rows // 2, 2 * lay
    vc = blk // CHUNKS
    n_z, n_y = lax.axis_size("gz"), lax.axis_size("gy")
    gz, gy = lax.axis_index("gz"), lax.axis_index("gy")
    p, group = gz % 2, gz // 2
    h = (p + gy) % 2
    partner = gz + 1 - 2 * p
    hs = pl.multiple_of(h * half, half)
    os = pl.multiple_of((1 - h) * half, half)
    mine_at = p * lay
    theirs_at = (1 - p) * lay
    below, above = group > 0, group < n_z // 2 - 1
    place = 2 * gy + h
    before, after = place > 0, place < 2 * n_y - 1
    prev_dev = (gz + h * (partner - gz), gy - (1 - h))
    next_dev = (gz + (1 - h) * (partner - gz), gy + h)
    basis = (k0, k1, k2, k3)
    edge = (lay - 1) * p

    def remote(src, dst, send, recv, dev):
        return pltpu.make_async_remote_copy(
            src_ref=src, dst_ref=dst, send_sem=send, recv_sem=recv, device_id=dev,
            device_id_type=MESH,
        )

    @pl.when(jnp.logical_not(below))
    def _():
        for k in (k0, k1, k2):
            k[:, 0] = jnp.zeros((blk, half, nx), jnp.float32)

    @pl.when(jnp.logical_not(above))
    def _():
        for k in (k0, k1, k2):
            k[:, group_lay + 1] = jnp.zeros((blk, half, nx), jnp.float32)

    @pl.when(jnp.logical_not(before))
    def _():
        yh[:, 0] = jnp.zeros((ITERS,) + yh.shape[2:], jnp.float32)

    @pl.when(jnp.logical_not(after))
    def _():
        yh[:, 1] = jnp.zeros((ITERS,) + yh.shape[2:], jnp.float32)

    barrier = pltpu.get_barrier_semaphore()
    for step in range(1, n_z):
        pl.semaphore_signal(
            barrier, inc=1, device_id=((gz + step) % n_z, gy), device_id_type=MESH
        )
    for step in range(1, n_y):
        pl.semaphore_signal(
            barrier, inc=1, device_id=(gz, (gy + step) % n_y), device_id_type=MESH
        )
    pl.semaphore_wait(barrier, n_z + n_y - 2)

    def exchange(which, ch):
        layer = edge + which * (1 - 2 * p)
        vs = pl.ds(ch * vc, vc)
        return remote(
            r_ref.at[vs, pl.ds(layer, 1), pl.ds(os, half)],
            k0.at[vs, pl.ds(1 + mine_at + layer, 1)],
            x_s.at[which, ch], x_r.at[which, ch], (partner, gy),
        )

    def z_from_rhs(ch, direction):
        vs = pl.ds(ch * vc, vc)
        if direction == 0:
            dst, dev = k0.at[vs, pl.ds(group_lay + 1, 1)], (gz - 2, gy)
        else:
            dst, dev = k0.at[vs, pl.ds(0, 1)], (gz + 2, gy)
        return remote(
            r_ref.at[vs, pl.ds(edge, 1), pl.ds(hs, half)], dst,
            z_s.at[0, direction, ch], z_r.at[0, direction, ch], dev,
        )

    def z_copy(j, ch, direction):
        vs = pl.ds(ch * vc, vc)
        k = basis[j]
        if direction == 0:
            src, dst, dev = k.at[vs, pl.ds(1, 1)], k.at[vs, pl.ds(group_lay + 1, 1)], (gz - 2, gy)
        else:
            src, dst, dev = k.at[vs, pl.ds(group_lay, 1)], k.at[vs, pl.ds(0, 1)], (gz + 2, gy)
        return remote(src, dst, z_s.at[j, direction, ch], z_r.at[j, direction, ch], dev)

    def y_copy(j, ch, side):
        vs = pl.ds(ch * vc, vc)
        dev = prev_dev if side == 0 else next_dev
        return remote(
            ys.at[j, side, vs], yh.at[j, 1 - side, vs],
            y_s.at[j, side, ch], y_r.at[j, 1 - side, ch], dev,
        )

    def y_wait_recv(j, ch, side):
        vs = pl.ds(ch * vc, vc)
        remote(
            ys.at[j, side, vs], yh.at[j, side, vs], y_s.at[j, side, ch], y_r.at[j, side, ch],
            (partner, gy),
        ).wait_recv()

    def back_copy(j, ch):
        vs = pl.ds(ch * vc, vc)
        dst = (ret1, ret2)[j - 1]
        return remote(
            basis[j].at[vs, pl.ds(1 + theirs_at, lay)], dst.at[vs],
            b_s.at[j - 1, ch], b_r.at[j - 1, ch], (partner, gy),
        )

    diag_copy = remote(
        d_ref.at[:, pl.ds(os, half)], diag.at[pl.ds(mine_at, lay)], d_s, d_r, (partner, gy)
    )

    def chunks(body):
        def run(ch, carry):
            body(ch)
            return carry

        lax.fori_loop(0, CHUNKS, run, 0)

    def first(ch):
        exchange(0, ch).start()

        @pl.when((p == 0) & below)
        def _():
            z_from_rhs(ch, 0).start()

        @pl.when((p == 1) & above)
        def _():
            z_from_rhs(ch, 1).start()

    chunks(first)
    chunks(lambda ch: exchange(1, ch).start())
    diag_copy.start()

    def own(v, carry):
        k0[v, pl.ds(1 + mine_at, lay)] = r_ref[v, :, pl.ds(hs, half)]
        return carry

    lax.fori_loop(0, blk, own, 0)
    diag[pl.ds(mine_at, lay)] = d_ref[:, pl.ds(hs, half)]

    lanes = nx // 128

    def gram(moment, left, right, l_at, r_at, layers, height):
        tiles = height // 8
        pairs = [(a, b) for a in range(blk) for b in range(a, blk)]

        def run(i, sums):
            layer, at = i // tiles, pl.multiple_of((i % tiles) * 8, 8)
            for lane in range(lanes):
                cols = pl.ds(lane * 128, 128)
                x = [left[v, l_at + layer, pl.ds(at, 8), cols] for v in range(blk)]
                y = x if left is right else [
                    right[v, r_at + layer, pl.ds(at, 8), cols] for v in range(blk)
                ]
                sums = tuple(s + x[a] * y[b] for s, (a, b) in zip(sums, pairs))
            return sums

        zero = jnp.zeros((8, 128), jnp.float32)
        sums = lax.fori_loop(0, layers * tiles, run, (zero,) * len(pairs))
        for s, (a, b) in zip(sums, pairs):
            line = jnp.sum(s, axis=0, keepdims=True)
            at = (moment * blk + a) * blk + b
            acc[at:at + 1] = line
            if a != b:
                at = (moment * blk + b) * blk + a
                acc[at:at + 1] = line

    acc[7 * blk * blk:] = jnp.zeros((acc.shape[0] - 7 * blk * blk, 128), jnp.float32)
    gram(0, r_ref, r_ref, 0, 0, lay, rows)

    def relay(ch):
        exchange_in = remote(
            r_ref.at[pl.ds(0, vc), pl.ds(0, 1), pl.ds(os, half)],
            k0.at[pl.ds(ch * vc, vc), pl.ds(1 + (group_lay - 1) * (1 - p), 1)],
            x_s.at[0, ch], x_r.at[0, ch], (partner, gy),
        )
        exchange_in.wait_recv()

        @pl.when((p == 0) & above)
        def _():
            z_copy(0, ch, 1).start()

        @pl.when((p == 1) & below)
        def _():
            z_copy(0, ch, 0).start()

    chunks(relay)

    def stage_rows(j, v, layer, value):
        ys[j, 0, v, layer:layer + 1] = value[:1]
        ys[j, 1, v, layer:layer + 1] = value[half - 1:]

    def start_rows(j, ch):
        @pl.when(before)
        def _():
            y_copy(j, ch, 0).start()

        @pl.when(after)
        def _():
            y_copy(j, ch, 1).start()

    def arrived(ch):
        remote(
            r_ref.at[pl.ds(0, vc), pl.ds(0, 1), pl.ds(os, half)],
            k0.at[pl.ds(ch * vc, vc), pl.ds(1 + lay - p, 1)],
            x_s.at[1, ch], x_r.at[1, ch], (partner, gy),
        ).wait_recv()

        def run(v, carry):
            for layer in range(group_lay):
                stage_rows(0, v, layer, k0[v, 1 + layer])
            return carry

        lax.fori_loop(ch * vc, (ch + 1) * vc, run, 0)
        start_rows(0, ch)

    chunks(arrived)
    remote(
        d_ref.at[:, pl.ds(os, half)], diag.at[pl.ds(theirs_at, lay)], d_s, d_r, (partner, gy)
    ).wait_recv()

    row_at = lax.broadcasted_iota(jnp.int32, (half, nx), 0)
    col_at = lax.broadcasted_iota(jnp.int32, (half, nx), 1)

    def step(j):
        src, dst = basis[j], basis[j + 1]
        shift = 0 if j == 2 else 1

        def apply(ch):
            @pl.when(below)
            def _():
                vs = pl.ds(ch * vc, vc)
                remote(
                    src.at[vs, pl.ds(1, 1)], src.at[vs, pl.ds(0, 1)],
                    z_s.at[j, 1, ch], z_r.at[j, 1, ch], (partner, gy),
                ).wait_recv()

            @pl.when(above)
            def _():
                vs = pl.ds(ch * vc, vc)
                remote(
                    src.at[vs, pl.ds(1, 1)], src.at[vs, pl.ds(group_lay + 1, 1)],
                    z_s.at[j, 0, ch], z_r.at[j, 0, ch], (partner, gy),
                ).wait_recv()

            @pl.when(before)
            def _():
                y_wait_recv(j, ch, 0)

            @pl.when(after)
            def _():
                y_wait_recv(j, ch, 1)

            def run(v, carry):
                for layer in range(group_lay):
                    here = src[v, 1 + layer]
                    near = src[v, layer] + src[v, 2 + layer]
                    up = jnp.where(
                        row_at == 0, yh[j, 0, v, layer:layer + 1], pltpu.roll(here, 1, 0)
                    )
                    down = jnp.where(
                        row_at == half - 1, yh[j, 1, v, layer:layer + 1],
                        pltpu.roll(here, half - 1, 0),
                    )
                    left = jnp.where(col_at == 0, 0.0, pltpu.roll(here, 1, 1))
                    right = jnp.where(col_at == nx - 1, 0.0, pltpu.roll(here, nx - 1, 1))
                    near = near + (up + down) + (left + right)
                    centre = (6.0 - CENTRE) + diag[layer]
                    value = SCALE * (centre * here - near)
                    dst[v, shift + layer] = value
                    if j < 2:
                        stage_rows(j + 1, v, layer, value)
                return carry

            lax.fori_loop(ch * vc, (ch + 1) * vc, run, 0)
            if j < 2:
                @pl.when(below)
                def _():
                    z_copy(j + 1, ch, 0).start()

                @pl.when(above)
                def _():
                    z_copy(j + 1, ch, 1).start()

                start_rows(j + 1, ch)
                back_copy(j + 1, ch).start()

        chunks(apply)
        gram(2 * j + 1, src, dst, 1, shift, group_lay, half)
        gram(2 * j + 2, dst, dst, shift, shift, group_lay, half)

    for j in range(ITERS):
        step(j)

    count = acc.shape[0]
    sums = nt_dot(jnp.ones((8, 128), jnp.float32), acc[...])
    lane_q = lax.broadcasted_iota(jnp.int32, (8, count), 1)
    row_q = lax.broadcasted_iota(jnp.int32, (8, count), 0)
    q = lax.broadcasted_iota(jnp.int32, (count, 128), 0)
    c = lax.broadcasted_iota(jnp.int32, (count, 128), 1)
    pick = (q // (blk * blk) == c // blk) & (q % blk == c % blk)
    kept = jnp.where((lane_q // blk) % blk == row_q, sums, 0.0)
    local = dot(kept, jnp.where(pick, 1.0, 0.0))
    mine[...] = local
    slots1[gy] = local

    def along(n, me, src, slots, send, recv, axis):
        at = (lambda i: (gz, i)) if axis == "gy" else (lambda i: (i, gy))
        for off in range(1, n):
            to = (me + off) % n
            remote(src, slots.at[me], send.at[to], recv.at[me], at(to)).start()
        for off in range(1, n):
            frm = (me + off) % n
            remote(src, slots.at[frm], send.at[frm], recv.at[frm], at(frm)).wait()
        total = slots[0]
        for i in range(1, n):
            total = total + slots[i]
        return total

    summed = along(n_y, gy, mine, slots1, g1_s, g1_r, "gy")
    part[...] = summed
    slots2[gz] = summed
    moments = along(n_z, gz, part, slots2, g2_s, g2_r, "gz")

    lane = lax.broadcasted_iota(jnp.int32, (8, 128), 1)
    keep = lambda x, low, high: jnp.where((lane >= low) & (lane < high), x, 0.0)
    left_by = lambda x, n: x if n == 0 else pltpu.roll(x, 128 - n, 1)
    order = (ITERS + 1) * blk
    lane32 = lax.broadcasted_iota(jnp.int32, (order, 128), 1)
    row32 = lax.broadcasted_iota(jnp.int32, (order, 128), 0)
    full = jnp.concatenate(
        [keep(left_by(moments, blk * i), 0, order) for i in range(ITERS + 1)], axis=0
    )
    full = full + jnp.where(lane32 == row32 + order, 1.0, 0.0)
    inv = 1.0 / SCALE
    second = (
        (inv * inv) * left_by(moments, 2 * blk)
        + (2.0 * CENTRE * inv) * left_by(moments, blk)
        + (CENTRE * CENTRE) * moments
    )
    target = inv * left_by(moments, blk) + CENTRE * moments
    small = ITERS * blk
    normal = jnp.concatenate(
        [
            keep(left_by(second, blk * i), 0, small)
            + keep(pltpu.roll(target, small - blk * i, 1) if i < ITERS else target, small, order)
            for i in range(ITERS)
        ],
        axis=0,
    )
    rows_small = lax.broadcasted_iota(jnp.int32, (small, 1), 0)
    rows_full = lax.broadcasted_iota(jnp.int32, (order, 1), 0)
    for k in range(order):
        if k < small:
            row = normal[k:k + 1] / normal[k:k + 1, k:k + 1]
            column = jnp.where(rows_small == k, 0.0, normal[:, k:k + 1])
            normal = jnp.where(rows_small == k, row, normal - column * row)
        row = full[k:k + 1] / full[k:k + 1, k:k + 1]
        column = jnp.where(rows_full <= k, 0.0, full[:, k:k + 1])
        full = full - column * row
    pivots = jnp.sum(jnp.where(lane32 == row32, full, 0.0), axis=1, keepdims=True)
    full = full / jnp.sqrt(pivots)
    upper = jnp.where((lane32 < order) & (lane32 >= row32), full, 0.0)
    lower_inv = left_by(full, order)
    lower_inv = jnp.where(lane32 < small, lower_inv, 0.0)[:small]
    hess = inv * nt_dot(pltpu.roll(lower_inv, blk, 1), upper)
    eye = lax.broadcasted_iota(jnp.int32, (small, order), 0) == lax.broadcasted_iota(
        jnp.int32, (small, order), 1
    )
    row_b = lax.broadcasted_iota(jnp.int32, (small, order), 0) // blk
    col_b = lax.broadcasted_iota(jnp.int32, (small, order), 1) // blk
    hess = hess + jnp.where(eye, CENTRE, 0.0)
    hess_ref[...] = jnp.where(col_b <= row_b + 1, hess, 0.0)

    for k in range(small):
        for u in range(blk):
            splat[k * blk + u] = jnp.broadcast_to(
                normal[k:k + 1, small + u:small + u + 1], (8, 128)
            )

    tiles = half // 8

    def combine(row_start, sources):
        def run(i, carry):
            layer, t = i // tiles, i % tiles
            at = pl.multiple_of(row_start + t * 8, 8)
            for lane_at in range(lanes):
                cols = pl.ds(lane_at * 128, 128)
                vals = []
                for ref, l_at, base in sources:
                    first_row = pl.multiple_of(base + t * 8, 8)
                    vals += [ref[v, l_at + layer, pl.ds(first_row, 8), cols] for v in range(blk)]
                for u in range(blk):
                    total = splat[u] * vals[0]
                    for k in range(1, small):
                        total = total + splat[k * blk + u] * vals[k]
                    out_ref[u, layer, pl.ds(at, 8), cols] = total
            return carry

        lax.fori_loop(0, lay * tiles, run, 0)

    combine(hs, ((r_ref, 0, hs), (k1, 1 + mine_at, 0), (k2, 1 + mine_at, 0)))

    def back_wait(ch):
        for j in (1, 2):
            back_copy(j, ch).wait()

    chunks(back_wait)
    combine(os, ((r_ref, 0, os), (ret1, 0, 0), (ret2, 0, 0)))

    def drain(ch):
        for which in (0, 1):
            exchange(which, ch).wait_send()
        for j in range(ITERS):
            @pl.when(below)
            def _():
                z_copy(j, ch, 0).wait_send()

            @pl.when(above)
            def _():
                z_copy(j, ch, 1).wait_send()

            @pl.when(before)
            def _():
                y_copy(j, ch, 0).wait_send()

            @pl.when(after)
            def _():
                y_copy(j, ch, 1).wait_send()

    chunks(drain)
    diag_copy.wait_send()


def body(right_side, diagonal):
    blk, lay, rows, nx = right_side.shape
    half, group_lay = rows // 2, 2 * lay
    n_z, n_y = lax.axis_size("gz"), lax.axis_size("gy")
    vmem = lambda *shape: pltpu.VMEM(shape, jnp.float32)
    dma = lambda *shape: pltpu.SemaphoreType.DMA(shape)
    small, order = ITERS * blk, (ITERS + 1) * blk
    return pl.pallas_call(
        kernel,
        out_shape=(
            jax.ShapeDtypeStruct(right_side.shape, jnp.float32),
            jax.ShapeDtypeStruct((small, order), jnp.float32),
        ),
        in_specs=[pl.BlockSpec(memory_space=pltpu.VMEM)] * 2,
        out_specs=(pl.BlockSpec(memory_space=pltpu.VMEM),) * 2,
        scratch_shapes=[
            vmem(blk, group_lay + 2, half, nx),
            vmem(blk, group_lay + 2, half, nx),
            vmem(blk, group_lay + 2, half, nx),
            vmem(blk, group_lay, half, nx),
            vmem(group_lay, half, nx),
            vmem(blk, lay, half, nx),
            vmem(blk, lay, half, nx),
            vmem(ITERS, 2, blk, group_lay, nx),
            vmem(ITERS, 2, blk, group_lay, nx),
            vmem(8 * blk * blk, 128),
            vmem(8, 128),
            vmem(n_y, 8, 128),
            vmem(8, 128),
            vmem(n_z, 8, 128),
            vmem(small * blk, 8, 128),
            dma(2, CHUNKS), dma(2, CHUNKS),
            pltpu.SemaphoreType.DMA, pltpu.SemaphoreType.DMA,
            dma(ITERS, 2, CHUNKS), dma(ITERS, 2, CHUNKS),
            dma(ITERS, 2, CHUNKS), dma(ITERS, 2, CHUNKS),
            dma(2, CHUNKS), dma(2, CHUNKS),
            dma(n_y), dma(n_y), dma(n_z), dma(n_z),
        ],
        compiler_params=pltpu.CompilerParams(
            collective_id=0, has_side_effects=True, vmem_limit_bytes=60 * 1024 * 1024
        ),
        name="gmres",
    )(right_side, diagonal)


def solution(mesh):
    in_specs = (P(None, "gz", "gy", None), P("gz", "gy", None))
    out_specs = (P(None, "gz", "gy", None), P())
    return jax.shard_map(body, mesh=mesh, in_specs=in_specs, out_specs=out_specs, check_vma=False)
```

```python
import functools

import jax
import jax.numpy as jnp
from jax import lax
from jax.experimental import pallas as pl
from jax.experimental.pallas import tpu as pltpu
from jax.sharding import PartitionSpec as P

ITERS = 3
CENTRE = 7.5
SCALE = 0.25
CHUNKS = 4
EARLY = 3
MESH = pl.DeviceIdType.MESH
HIGH = lax.Precision.HIGHEST


def nt_dot(left, right):
    return lax.dot_general(
        left, right, (((1,), (1,)), ((), ())), precision=HIGH, preferred_element_type=jnp.float32
    )


def dot(left, right):
    return jnp.dot(left, right, precision=HIGH, preferred_element_type=jnp.float32)


def kernel(
    r_ref, d_ref, out_ref, hess_ref,
    k0, k1, k2, k3, diag, ret1, ret2, held, ys, yh, acc, mine, slots1, part, slots2, splat,
    x_s, x_r, d_s, d_r, z_s, z_r, y_s, y_r, b_s, b_r, l_s, l_r, g1_s, g1_r, g2_s, g2_r,
):
    blk, lay, rows, nx = r_ref.shape
    half, group_lay = rows // 2, 2 * lay
    vc = blk // CHUNKS
    n_z, n_y = lax.axis_size("gz"), lax.axis_size("gy")
    gz, gy = lax.axis_index("gz"), lax.axis_index("gy")
    p, group = gz % 2, gz // 2
    h = (p + gy) % 2
    partner = gz + 1 - 2 * p
    hs = pl.multiple_of(h * half, half)
    os = pl.multiple_of((1 - h) * half, half)
    mine_at = p * lay
    theirs_at = (1 - p) * lay
    below, above = group > 0, group < n_z // 2 - 1
    place = 2 * gy + h
    before, after = place > 0, place < 2 * n_y - 1
    prev_dev = (gz + h * (partner - gz), gy - (1 - h))
    next_dev = (gz + (1 - h) * (partner - gz), gy + h)
    basis = (k0, k1, k2, k3)
    edge = (lay - 1) * p

    def remote(src, dst, send, recv, dev):
        return pltpu.make_async_remote_copy(
            src_ref=src, dst_ref=dst, send_sem=send, recv_sem=recv, device_id=dev,
            device_id_type=MESH,
        )

    @pl.when(jnp.logical_not(below))
    def _():
        for k in (k0, k1, k2):
            k[:, 0] = jnp.zeros((blk, half, nx), jnp.float32)

    @pl.when(jnp.logical_not(above))
    def _():
        for k in (k0, k1, k2):
            k[:, group_lay + 1] = jnp.zeros((blk, half, nx), jnp.float32)

    @pl.when(jnp.logical_not(before))
    def _():
        yh[:, 0] = jnp.zeros((ITERS,) + yh.shape[2:], jnp.float32)

    @pl.when(jnp.logical_not(after))
    def _():
        yh[:, 1] = jnp.zeros((ITERS,) + yh.shape[2:], jnp.float32)

    barrier = pltpu.get_barrier_semaphore()
    for step in range(1, n_z):
        pl.semaphore_signal(
            barrier, inc=1, device_id=((gz + step) % n_z, gy), device_id_type=MESH
        )
    for step in range(1, n_y):
        pl.semaphore_signal(
            barrier, inc=1, device_id=(gz, (gy + step) % n_y), device_id_type=MESH
        )
    pl.semaphore_wait(barrier, n_z + n_y - 2)

    def exchange(which, ch):
        layer = edge + which * (1 - 2 * p)
        vs = pl.ds(ch * vc, vc)
        return remote(
            r_ref.at[vs, pl.ds(layer, 1), pl.ds(os, half)],
            k0.at[vs, pl.ds(1 + mine_at + layer, 1)],
            x_s.at[which, ch], x_r.at[which, ch], (partner, gy),
        )

    def z_from_rhs(ch, direction):
        vs = pl.ds(ch * vc, vc)
        if direction == 0:
            dst, dev = k0.at[vs, pl.ds(group_lay + 1, 1)], (gz - 2, gy)
        else:
            dst, dev = k0.at[vs, pl.ds(0, 1)], (gz + 2, gy)
        return remote(
            r_ref.at[vs, pl.ds(edge, 1), pl.ds(hs, half)], dst,
            z_s.at[0, direction, ch], z_r.at[0, direction, ch], dev,
        )

    def z_copy(j, ch, direction):
        vs = pl.ds(ch * vc, vc)
        k = basis[j]
        if direction == 0:
            src, dst, dev = k.at[vs, pl.ds(1, 1)], k.at[vs, pl.ds(group_lay + 1, 1)], (gz - 2, gy)
        else:
            src, dst, dev = k.at[vs, pl.ds(group_lay, 1)], k.at[vs, pl.ds(0, 1)], (gz + 2, gy)
        return remote(src, dst, z_s.at[j, direction, ch], z_r.at[j, direction, ch], dev)

    def y_copy(j, ch, side):
        vs = pl.ds(ch * vc, vc)
        dev = prev_dev if side == 0 else next_dev
        return remote(
            ys.at[j, side, vs], yh.at[j, 1 - side, vs],
            y_s.at[j, side, ch], y_r.at[j, 1 - side, ch], dev,
        )

    def y_wait_recv(j, ch, side):
        vs = pl.ds(ch * vc, vc)
        remote(
            ys.at[j, side, vs], yh.at[j, side, vs], y_s.at[j, side, ch], y_r.at[j, side, ch],
            (partner, gy),
        ).wait_recv()

    early = ret1.shape[2]
    late = half - early

    def back_copy(j, ch, layer):
        vs = pl.ds(ch * vc, vc)
        dst = (ret1, ret2)[j - 1]
        return remote(
            basis[j].at[vs, pl.ds(1 + theirs_at + layer, 1), pl.ds(0, early)],
            dst.at[vs, pl.ds(layer, 1)],
            b_s.at[j - 1, layer, ch], b_r.at[j - 1, layer, ch], (partner, gy),
        )

    def late_copy(layer):
        return remote(
            held.at[:, pl.ds(layer, 1)],
            out_ref.at[:, pl.ds(layer, 1), pl.ds(pl.multiple_of(hs + early, 8), late)],
            l_s.at[layer], l_r.at[layer], (partner, gy),
        )

    diag_copy = remote(
        d_ref.at[:, pl.ds(os, half)], diag.at[pl.ds(mine_at, lay)], d_s, d_r, (partner, gy)
    )

    def chunks(body):
        def run(ch, carry):
            body(ch)
            return carry

        lax.fori_loop(0, CHUNKS, run, 0)

    def first(ch):
        exchange(0, ch).start()

        @pl.when((p == 0) & below)
        def _():
            z_from_rhs(ch, 0).start()

        @pl.when((p == 1) & above)
        def _():
            z_from_rhs(ch, 1).start()

    chunks(first)
    chunks(lambda ch: exchange(1, ch).start())
    diag_copy.start()

    def own(v, carry):
        k0[v, pl.ds(1 + mine_at, lay)] = r_ref[v, :, pl.ds(hs, half)]
        return carry

    lax.fori_loop(0, blk, own, 0)
    diag[pl.ds(mine_at, lay)] = d_ref[:, pl.ds(hs, half)]

    lanes = nx // 128

    def gram(moment, left, right, l_at, r_at, layers, height):
        tiles = height // 8
        pairs = [(a, b) for a in range(blk) for b in range(a, blk)]

        def run(i, sums):
            layer, at = i // tiles, pl.multiple_of((i % tiles) * 8, 8)
            for lane in range(lanes):
                cols = pl.ds(lane * 128, 128)
                x = [left[v, l_at + layer, pl.ds(at, 8), cols] for v in range(blk)]
                y = x if left is right else [
                    right[v, r_at + layer, pl.ds(at, 8), cols] for v in range(blk)
                ]
                sums = tuple(s + x[a] * y[b] for s, (a, b) in zip(sums, pairs))
            return sums

        zero = jnp.zeros((8, 128), jnp.float32)
        sums = lax.fori_loop(0, layers * tiles, run, (zero,) * len(pairs))
        for s, (a, b) in zip(sums, pairs):
            line = jnp.sum(s, axis=0, keepdims=True)
            at = (moment * blk + a) * blk + b
            acc[at:at + 1] = line
            if a != b:
                at = (moment * blk + b) * blk + a
                acc[at:at + 1] = line

    acc[7 * blk * blk:] = jnp.zeros((acc.shape[0] - 7 * blk * blk, 128), jnp.float32)
    gram(0, r_ref, r_ref, 0, 0, lay, rows)

    def relay(ch):
        exchange_in = remote(
            r_ref.at[pl.ds(0, vc), pl.ds(0, 1), pl.ds(os, half)],
            k0.at[pl.ds(ch * vc, vc), pl.ds(1 + (group_lay - 1) * (1 - p), 1)],
            x_s.at[0, ch], x_r.at[0, ch], (partner, gy),
        )
        exchange_in.wait_recv()

        @pl.when((p == 0) & above)
        def _():
            z_copy(0, ch, 1).start()

        @pl.when((p == 1) & below)
        def _():
            z_copy(0, ch, 0).start()

    chunks(relay)

    def stage_rows(j, v, layer, value):
        ys[j, 0, v, layer:layer + 1] = value[:1]
        ys[j, 1, v, layer:layer + 1] = value[half - 1:]

    def start_rows(j, ch):
        @pl.when(before)
        def _():
            y_copy(j, ch, 0).start()

        @pl.when(after)
        def _():
            y_copy(j, ch, 1).start()

    def arrived(ch):
        remote(
            r_ref.at[pl.ds(0, vc), pl.ds(0, 1), pl.ds(os, half)],
            k0.at[pl.ds(ch * vc, vc), pl.ds(1 + lay - p, 1)],
            x_s.at[1, ch], x_r.at[1, ch], (partner, gy),
        ).wait_recv()

        def run(v, carry):
            for layer in range(group_lay):
                stage_rows(0, v, layer, k0[v, 1 + layer])
            return carry

        lax.fori_loop(ch * vc, (ch + 1) * vc, run, 0)
        start_rows(0, ch)

    chunks(arrived)
    remote(
        d_ref.at[:, pl.ds(os, half)], diag.at[pl.ds(theirs_at, lay)], d_s, d_r, (partner, gy)
    ).wait_recv()

    row_at = lax.broadcasted_iota(jnp.int32, (half, nx), 0)
    col_at = lax.broadcasted_iota(jnp.int32, (half, nx), 1)

    def step(j):
        src, dst = basis[j], basis[j + 1]
        shift = 0 if j == 2 else 1

        def apply(ch):
            @pl.when(below)
            def _():
                vs = pl.ds(ch * vc, vc)
                remote(
                    src.at[vs, pl.ds(1, 1)], src.at[vs, pl.ds(0, 1)],
                    z_s.at[j, 1, ch], z_r.at[j, 1, ch], (partner, gy),
                ).wait_recv()

            @pl.when(above)
            def _():
                vs = pl.ds(ch * vc, vc)
                remote(
                    src.at[vs, pl.ds(1, 1)], src.at[vs, pl.ds(group_lay + 1, 1)],
                    z_s.at[j, 0, ch], z_r.at[j, 0, ch], (partner, gy),
                ).wait_recv()

            @pl.when(before)
            def _():
                y_wait_recv(j, ch, 0)

            @pl.when(after)
            def _():
                y_wait_recv(j, ch, 1)

            def run(v, carry):
                for layer in range(group_lay):
                    here = src[v, 1 + layer]
                    near = src[v, layer] + src[v, 2 + layer]
                    up = jnp.where(
                        row_at == 0, yh[j, 0, v, layer:layer + 1], pltpu.roll(here, 1, 0)
                    )
                    down = jnp.where(
                        row_at == half - 1, yh[j, 1, v, layer:layer + 1],
                        pltpu.roll(here, half - 1, 0),
                    )
                    left = jnp.where(col_at == 0, 0.0, pltpu.roll(here, 1, 1))
                    right = jnp.where(col_at == nx - 1, 0.0, pltpu.roll(here, nx - 1, 1))
                    near = near + (up + down) + (left + right)
                    centre = (6.0 - CENTRE) + diag[layer]
                    value = SCALE * (centre * here - near)
                    dst[v, shift + layer] = value
                    if j < 2:
                        stage_rows(j + 1, v, layer, value)
                return carry

            lax.fori_loop(ch * vc, (ch + 1) * vc, run, 0)
            if j < 2:
                @pl.when(below)
                def _():
                    z_copy(j + 1, ch, 0).start()

                @pl.when(above)
                def _():
                    z_copy(j + 1, ch, 1).start()

                start_rows(j + 1, ch)
            if j == 0:
                for layer in range(lay // 2):
                    back_copy(1, ch, layer).start()
            elif j == 1:
                for layer in range(lay // 2, lay):
                    back_copy(1, ch, layer).start()
            else:
                for layer in range(lay):
                    back_copy(2, ch, layer).start()

        chunks(apply)
        gram(2 * j + 1, src, dst, 1, shift, group_lay, half)
        gram(2 * j + 2, dst, dst, shift, shift, group_lay, half)

    for j in range(ITERS):
        step(j)

    count = acc.shape[0]
    sums = nt_dot(jnp.ones((8, 128), jnp.float32), acc[...])
    lane_q = lax.broadcasted_iota(jnp.int32, (8, count), 1)
    row_q = lax.broadcasted_iota(jnp.int32, (8, count), 0)
    q = lax.broadcasted_iota(jnp.int32, (count, 128), 0)
    c = lax.broadcasted_iota(jnp.int32, (count, 128), 1)
    pick = (q // (blk * blk) == c // blk) & (q % blk == c % blk)
    kept = jnp.where((lane_q // blk) % blk == row_q, sums, 0.0)
    local = dot(kept, jnp.where(pick, 1.0, 0.0))
    mine[...] = local
    slots1[gy] = local

    def along(n, me, src, slots, send, recv, axis):
        at = (lambda i: (gz, i)) if axis == "gy" else (lambda i: (i, gy))
        for off in range(1, n):
            to = (me + off) % n
            remote(src, slots.at[me], send.at[to], recv.at[me], at(to)).start()
        for off in range(1, n):
            frm = (me + off) % n
            remote(src, slots.at[frm], send.at[frm], recv.at[frm], at(frm)).wait()
        total = slots[0]
        for i in range(1, n):
            total = total + slots[i]
        return total

    summed = along(n_y, gy, mine, slots1, g1_s, g1_r, "gy")
    part[...] = summed
    slots2[gz] = summed
    moments = along(n_z, gz, part, slots2, g2_s, g2_r, "gz")

    lane = lax.broadcasted_iota(jnp.int32, (8, 128), 1)
    keep = lambda x, low, high: jnp.where((lane >= low) & (lane < high), x, 0.0)
    left_by = lambda x, n: x if n == 0 else pltpu.roll(x, 128 - n, 1)
    order = (ITERS + 1) * blk
    lane32 = lax.broadcasted_iota(jnp.int32, (order, 128), 1)
    row32 = lax.broadcasted_iota(jnp.int32, (order, 128), 0)
    full = jnp.concatenate(
        [keep(left_by(moments, blk * i), 0, order) for i in range(ITERS + 1)], axis=0
    )
    full = full + jnp.where(lane32 == row32 + order, 1.0, 0.0)
    inv = 1.0 / SCALE
    second = (
        (inv * inv) * left_by(moments, 2 * blk)
        + (2.0 * CENTRE * inv) * left_by(moments, blk)
        + (CENTRE * CENTRE) * moments
    )
    target = inv * left_by(moments, blk) + CENTRE * moments
    small = ITERS * blk
    normal = jnp.concatenate(
        [
            keep(left_by(second, blk * i), 0, small)
            + keep(pltpu.roll(target, small - blk * i, 1) if i < ITERS else target, small, order)
            for i in range(ITERS)
        ],
        axis=0,
    )
    rows_small = lax.broadcasted_iota(jnp.int32, (small, 1), 0)
    rows_full = lax.broadcasted_iota(jnp.int32, (order, 1), 0)
    for k in range(order):
        if k < small:
            row = normal[k:k + 1] / normal[k:k + 1, k:k + 1]
            column = jnp.where(rows_small == k, 0.0, normal[:, k:k + 1])
            normal = jnp.where(rows_small == k, row, normal - column * row)
        row = full[k:k + 1] / full[k:k + 1, k:k + 1]
        column = jnp.where(rows_full <= k, 0.0, full[:, k:k + 1])
        full = full - column * row
    pivots = jnp.sum(jnp.where(lane32 == row32, full, 0.0), axis=1, keepdims=True)
    full = full / jnp.sqrt(pivots)
    upper = jnp.where((lane32 < order) & (lane32 >= row32), full, 0.0)
    lower_inv = left_by(full, order)
    lower_inv = jnp.where(lane32 < small, lower_inv, 0.0)[:small]
    hess = inv * nt_dot(pltpu.roll(lower_inv, blk, 1), upper)
    eye = lax.broadcasted_iota(jnp.int32, (small, order), 0) == lax.broadcasted_iota(
        jnp.int32, (small, order), 1
    )
    row_b = lax.broadcasted_iota(jnp.int32, (small, order), 0) // blk
    col_b = lax.broadcasted_iota(jnp.int32, (small, order), 1) // blk
    hess = hess + jnp.where(eye, CENTRE, 0.0)
    hess_ref[...] = jnp.where(col_b <= row_b + 1, hess, 0.0)

    for k in range(small):
        for u in range(blk):
            splat[k * blk + u] = jnp.broadcast_to(
                normal[k:k + 1, small + u:small + u + 1], (8, 128)
            )

    def combine(dst, layers, row_start, height, sources):
        tiles = height // 8

        def run(i, carry):
            layer, t = layers[0] + i // tiles, i % tiles
            at = pl.multiple_of(row_start + t * 8, 8)
            for lane_at in range(lanes):
                cols = pl.ds(lane_at * 128, 128)
                vals = []
                for ref, l_at, base in sources:
                    first_row = pl.multiple_of(base + t * 8, 8)
                    vals += [ref[v, l_at + layer, pl.ds(first_row, 8), cols] for v in range(blk)]
                for u in range(blk):
                    total = splat[u] * vals[0]
                    for k in range(1, small):
                        total = total + splat[k * blk + u] * vals[k]
                    dst[u, layer, pl.ds(at, 8), cols] = total
            return carry

        lax.fori_loop(0, (layers[1] - layers[0]) * tiles, run, 0)

    for layer in range(lay):
        combine(held, (layer, layer + 1), 0, late, [(k, 1 + theirs_at, early) for k in basis[:ITERS]])
        late_copy(layer).start()
    combine(
        out_ref, (0, lay), hs, half, ((r_ref, 0, hs), (k1, 1 + mine_at, 0), (k2, 1 + mine_at, 0))
    )

    def back_wait(ch):
        for j in (1, 2):
            for layer in range(lay):
                back_copy(j, ch, layer).wait()

    chunks(back_wait)
    combine(out_ref, (0, lay), os, early, ((r_ref, 0, os), (ret1, 0, 0), (ret2, 0, 0)))
    for layer in range(lay):
        late_copy(layer).wait_send()
        remote(
            held.at[:, pl.ds(layer, 1)],
            out_ref.at[:, pl.ds(layer, 1), pl.ds(pl.multiple_of(os + early, 8), late)],
            l_s.at[layer], l_r.at[layer], (partner, gy),
        ).wait_recv()

    def drain(ch):
        for which in (0, 1):
            exchange(which, ch).wait_send()
        for j in range(ITERS):
            @pl.when(below)
            def _():
                z_copy(j, ch, 0).wait_send()

            @pl.when(above)
            def _():
                z_copy(j, ch, 1).wait_send()

            @pl.when(before)
            def _():
                y_copy(j, ch, 0).wait_send()

            @pl.when(after)
            def _():
                y_copy(j, ch, 1).wait_send()

    chunks(drain)
    diag_copy.wait_send()


def body(right_side, diagonal):
    blk, lay, rows, nx = right_side.shape
    half, group_lay = rows // 2, 2 * lay
    early = half * EARLY // 32 * 8
    n_z, n_y = lax.axis_size("gz"), lax.axis_size("gy")
    vmem = lambda *shape: pltpu.VMEM(shape, jnp.float32)
    dma = lambda *shape: pltpu.SemaphoreType.DMA(shape)
    small, order = ITERS * blk, (ITERS + 1) * blk
    return pl.pallas_call(
        kernel,
        out_shape=(
            jax.ShapeDtypeStruct(right_side.shape, jnp.float32),
            jax.ShapeDtypeStruct((small, order), jnp.float32),
        ),
        in_specs=[pl.BlockSpec(memory_space=pltpu.VMEM)] * 2,
        out_specs=(pl.BlockSpec(memory_space=pltpu.VMEM),) * 2,
        scratch_shapes=[
            vmem(blk, group_lay + 2, half, nx),
            vmem(blk, group_lay + 2, half, nx),
            vmem(blk, group_lay + 2, half, nx),
            vmem(blk, group_lay, half, nx),
            vmem(group_lay, half, nx),
            vmem(blk, lay, early, nx),
            vmem(blk, lay, early, nx),
            vmem(blk, lay, half - early, nx),
            vmem(ITERS, 2, blk, group_lay, nx),
            vmem(ITERS, 2, blk, group_lay, nx),
            vmem(8 * blk * blk, 128),
            vmem(8, 128),
            vmem(n_y, 8, 128),
            vmem(8, 128),
            vmem(n_z, 8, 128),
            vmem(small * blk, 8, 128),
            dma(2, CHUNKS), dma(2, CHUNKS),
            pltpu.SemaphoreType.DMA, pltpu.SemaphoreType.DMA,
            dma(ITERS, 2, CHUNKS), dma(ITERS, 2, CHUNKS),
            dma(ITERS, 2, CHUNKS), dma(ITERS, 2, CHUNKS),
            dma(2, lay, CHUNKS), dma(2, lay, CHUNKS), dma(lay), dma(lay),
            dma(n_y), dma(n_y), dma(n_z), dma(n_z),
        ],
        compiler_params=pltpu.CompilerParams(
            collective_id=0, has_side_effects=True, vmem_limit_bytes=60 * 1024 * 1024
        ),
        name="gmres",
    )(right_side, diagonal)


def solution(mesh):
    in_specs = (P(None, "gz", "gy", None), P("gz", "gy", None))
    out_specs = (P(None, "gz", "gy", None), P())
    return jax.shard_map(body, mesh=mesh, in_specs=in_specs, out_specs=out_specs, check_vma=False)
```

```python
import functools

import jax
import jax.numpy as jnp
from jax import lax
from jax.experimental import pallas as pl
from jax.experimental.pallas import tpu as pltpu
from jax.sharding import PartitionSpec as P

ITERS = 3
CENTRE = 7.5
SCALE = 0.25
CHUNKS = 8
AHEAD = 2
EARLY = 2
MESH = pl.DeviceIdType.MESH
HIGH = lax.Precision.HIGHEST


def nt_dot(left, right):
    return lax.dot_general(
        left, right, (((1,), (1,)), ((), ())), precision=HIGH, preferred_element_type=jnp.float32
    )


def dot(left, right):
    return jnp.dot(left, right, precision=HIGH, preferred_element_type=jnp.float32)


def kernel(
    r_ref, d_ref, out_ref, hess_ref,
    k0, k1, k2, k3, diag, ret1, ret2, held, ys, yh, acc, mine, slots1, part, slots2, splat,
    x_s, x_r, d_s, d_r, z_s, z_r, y_s, y_r, b_s, b_r, l_s, l_r, g1_s, g1_r, g2_s, g2_r,
):
    blk, lay, rows, nx = r_ref.shape
    half, group_lay = rows // 2, 2 * lay
    vc = blk // CHUNKS
    n_z, n_y = lax.axis_size("gz"), lax.axis_size("gy")
    gz, gy = lax.axis_index("gz"), lax.axis_index("gy")
    p, group = gz % 2, gz // 2
    h = (p + gy) % 2
    partner = gz + 1 - 2 * p
    hs = pl.multiple_of(h * half, half)
    os = pl.multiple_of((1 - h) * half, half)
    mine_at = p * lay
    theirs_at = (1 - p) * lay
    below, above = group > 0, group < n_z // 2 - 1
    place = 2 * gy + h
    before, after = place > 0, place < 2 * n_y - 1
    prev_dev = (gz + h * (partner - gz), gy - (1 - h))
    next_dev = (gz + (1 - h) * (partner - gz), gy + h)
    basis = (k0, k1, k2, k3)
    edge = (lay - 1) * p

    def remote(src, dst, send, recv, dev):
        return pltpu.make_async_remote_copy(
            src_ref=src, dst_ref=dst, send_sem=send, recv_sem=recv, device_id=dev,
            device_id_type=MESH,
        )

    @pl.when(jnp.logical_not(below))
    def _():
        for k in (k0, k1, k2):
            k[:, 0] = jnp.zeros((blk, half, nx), jnp.float32)

    @pl.when(jnp.logical_not(above))
    def _():
        for k in (k0, k1, k2):
            k[:, group_lay + 1] = jnp.zeros((blk, half, nx), jnp.float32)

    @pl.when(jnp.logical_not(before))
    def _():
        yh[:, 0] = jnp.zeros((ITERS,) + yh.shape[2:], jnp.float32)

    @pl.when(jnp.logical_not(after))
    def _():
        yh[:, 1] = jnp.zeros((ITERS,) + yh.shape[2:], jnp.float32)

    barrier = pltpu.get_barrier_semaphore()
    for step in range(1, n_z):
        pl.semaphore_signal(
            barrier, inc=1, device_id=((gz + step) % n_z, gy), device_id_type=MESH
        )
    for step in range(1, n_y):
        pl.semaphore_signal(
            barrier, inc=1, device_id=(gz, (gy + step) % n_y), device_id_type=MESH
        )
    pl.semaphore_wait(barrier, n_z + n_y - 2)

    def exchange(which, ch):
        layer = edge + which * (1 - 2 * p)
        vs = pl.ds(ch * vc, vc)
        return remote(
            r_ref.at[vs, pl.ds(layer, 1), pl.ds(os, half)],
            k0.at[vs, pl.ds(1 + mine_at + layer, 1)],
            x_s.at[which, ch], x_r.at[which, ch], (partner, gy),
        )

    def z_from_rhs(ch, direction):
        vs = pl.ds(ch * vc, vc)
        if direction == 0:
            dst, dev = k0.at[vs, pl.ds(group_lay + 1, 1)], (gz - 2, gy)
        else:
            dst, dev = k0.at[vs, pl.ds(0, 1)], (gz + 2, gy)
        return remote(
            r_ref.at[vs, pl.ds(edge, 1), pl.ds(hs, half)], dst,
            z_s.at[0, direction, ch], z_r.at[0, direction, ch], dev,
        )

    def z_copy(j, ch, direction):
        vs = pl.ds(ch * vc, vc)
        k = basis[j]
        if direction == 0:
            src, dst, dev = k.at[vs, pl.ds(1, 1)], k.at[vs, pl.ds(group_lay + 1, 1)], (gz - 2, gy)
        else:
            src, dst, dev = k.at[vs, pl.ds(group_lay, 1)], k.at[vs, pl.ds(0, 1)], (gz + 2, gy)
        return remote(src, dst, z_s.at[j, direction, ch], z_r.at[j, direction, ch], dev)

    def y_copy(j, ch, side):
        vs = pl.ds(ch * vc, vc)
        dev = prev_dev if side == 0 else next_dev
        return remote(
            ys.at[j, side, vs], yh.at[j, 1 - side, vs],
            y_s.at[j, side, ch], y_r.at[j, 1 - side, ch], dev,
        )

    def y_wait_recv(j, ch, side):
        vs = pl.ds(ch * vc, vc)
        remote(
            ys.at[j, side, vs], yh.at[j, side, vs], y_s.at[j, side, ch], y_r.at[j, side, ch],
            (partner, gy),
        ).wait_recv()

    early = ret1.shape[2]
    late = half - early

    def back_copy(j, ch, layer):
        vs = pl.ds(ch * vc, vc)
        dst = (ret1, ret2)[j - 1]
        return remote(
            basis[j].at[vs, pl.ds(1 + theirs_at + layer, 1), pl.ds(0, early)],
            dst.at[vs, pl.ds(layer, 1)],
            b_s.at[j - 1, layer, ch], b_r.at[j - 1, layer, ch], (partner, gy),
        )

    def late_copy(layer):
        return remote(
            held.at[:, pl.ds(layer, 1)],
            out_ref.at[:, pl.ds(layer, 1), pl.ds(pl.multiple_of(hs + early, 8), late)],
            l_s.at[layer], l_r.at[layer], (partner, gy),
        )

    diag_copy = remote(
        d_ref.at[:, pl.ds(os, half)], diag.at[pl.ds(mine_at, lay)], d_s, d_r, (partner, gy)
    )

    def chunks(body):
        def run(ch, carry):
            body(ch)
            return carry

        lax.fori_loop(0, CHUNKS, run, 0)

    def first(ch):
        exchange(0, ch).start()
        exchange(1, ch).start()

        @pl.when((p == 0) & below)
        def _():
            z_from_rhs(ch, 0).start()

        @pl.when((p == 1) & above)
        def _():
            z_from_rhs(ch, 1).start()

    first(0)
    diag_copy.start()
    for ch in range(1, AHEAD):
        first(ch)

    def own(v, carry):
        k0[v, pl.ds(1 + mine_at, lay)] = r_ref[v, :, pl.ds(hs, half)]
        return carry

    lax.fori_loop(0, blk, own, 0)
    diag[pl.ds(mine_at, lay)] = d_ref[:, pl.ds(hs, half)]

    lanes = nx // 128

    def gram(moment, left, right, l_at, r_at, layers, height):
        tiles = height // 8
        pairs = [(a, b) for a in range(blk) for b in range(a, blk)]

        def run(i, sums):
            layer, at = i // tiles, pl.multiple_of((i % tiles) * 8, 8)
            for lane in range(lanes):
                cols = pl.ds(lane * 128, 128)
                x = [left[v, l_at + layer, pl.ds(at, 8), cols] for v in range(blk)]
                y = x if left is right else [
                    right[v, r_at + layer, pl.ds(at, 8), cols] for v in range(blk)
                ]
                sums = tuple(s + x[a] * y[b] for s, (a, b) in zip(sums, pairs))
            return sums

        zero = jnp.zeros((8, 128), jnp.float32)
        sums = lax.fori_loop(0, layers * tiles, run, (zero,) * len(pairs))
        for s, (a, b) in zip(sums, pairs):
            line = jnp.sum(s, axis=0, keepdims=True)
            at = (moment * blk + a) * blk + b
            acc[at:at + 1] = line
            if a != b:
                at = (moment * blk + b) * blk + a
                acc[at:at + 1] = line

    acc[7 * blk * blk:] = jnp.zeros((acc.shape[0] - 7 * blk * blk, 128), jnp.float32)
    gram(0, r_ref, r_ref, 0, 0, lay, rows)

    def relay(ch):
        exchange_in = remote(
            r_ref.at[pl.ds(0, vc), pl.ds(0, 1), pl.ds(os, half)],
            k0.at[pl.ds(ch * vc, vc), pl.ds(1 + (group_lay - 1) * (1 - p), 1)],
            x_s.at[0, ch], x_r.at[0, ch], (partner, gy),
        )
        exchange_in.wait_recv()

        @pl.when((p == 0) & above)
        def _():
            z_copy(0, ch, 1).start()

        @pl.when((p == 1) & below)
        def _():
            z_copy(0, ch, 0).start()

    def stage_rows(j, v, layer, value):
        ys[j, 0, v, layer:layer + 1] = value[:1]
        ys[j, 1, v, layer:layer + 1] = value[half - 1:]

    def start_rows(j, ch):
        @pl.when(before)
        def _():
            y_copy(j, ch, 0).start()

        @pl.when(after)
        def _():
            y_copy(j, ch, 1).start()

    def arrived(ch):
        remote(
            r_ref.at[pl.ds(0, vc), pl.ds(0, 1), pl.ds(os, half)],
            k0.at[pl.ds(ch * vc, vc), pl.ds(1 + lay - p, 1)],
            x_s.at[1, ch], x_r.at[1, ch], (partner, gy),
        ).wait_recv()

        def run(v, carry):
            for layer in range(group_lay):
                stage_rows(0, v, layer, k0[v, 1 + layer])
            return carry

        lax.fori_loop(ch * vc, (ch + 1) * vc, run, 0)
        start_rows(0, ch)

    def diag_arrived():
        remote(
            d_ref.at[:, pl.ds(os, half)], diag.at[pl.ds(theirs_at, lay)], d_s, d_r, (partner, gy)
        ).wait_recv()

    row_at = lax.broadcasted_iota(jnp.int32, (half, nx), 0)
    col_at = lax.broadcasted_iota(jnp.int32, (half, nx), 1)

    def apply(j, ch):
        src, dst = basis[j], basis[j + 1]
        shift = 0 if j == 2 else 1

        if True:
            @pl.when(below)
            def _():
                vs = pl.ds(ch * vc, vc)
                remote(
                    src.at[vs, pl.ds(1, 1)], src.at[vs, pl.ds(0, 1)],
                    z_s.at[j, 1, ch], z_r.at[j, 1, ch], (partner, gy),
                ).wait_recv()

            @pl.when(above)
            def _():
                vs = pl.ds(ch * vc, vc)
                remote(
                    src.at[vs, pl.ds(1, 1)], src.at[vs, pl.ds(group_lay + 1, 1)],
                    z_s.at[j, 0, ch], z_r.at[j, 0, ch], (partner, gy),
                ).wait_recv()

            @pl.when(before)
            def _():
                y_wait_recv(j, ch, 0)

            @pl.when(after)
            def _():
                y_wait_recv(j, ch, 1)

            def run(v, carry):
                for layer in range(group_lay):
                    here = src[v, 1 + layer]
                    near = src[v, layer] + src[v, 2 + layer]
                    up = jnp.where(
                        row_at == 0, yh[j, 0, v, layer:layer + 1], pltpu.roll(here, 1, 0)
                    )
                    down = jnp.where(
                        row_at == half - 1, yh[j, 1, v, layer:layer + 1],
                        pltpu.roll(here, half - 1, 0),
                    )
                    left = jnp.where(col_at == 0, 0.0, pltpu.roll(here, 1, 1))
                    right = jnp.where(col_at == nx - 1, 0.0, pltpu.roll(here, nx - 1, 1))
                    near = near + (up + down) + (left + right)
                    centre = (6.0 - CENTRE) + diag[layer]
                    value = SCALE * (centre * here - near)
                    dst[v, shift + layer] = value
                    if j < 2:
                        stage_rows(j + 1, v, layer, value)
                return carry

            lax.fori_loop(ch * vc, (ch + 1) * vc, run, 0)
            if j < 2:
                @pl.when(below)
                def _():
                    z_copy(j + 1, ch, 0).start()

                @pl.when(above)
                def _():
                    z_copy(j + 1, ch, 1).start()

                start_rows(j + 1, ch)

    def grams(j):
        shift = 0 if j == 2 else 1
        gram(2 * j + 1, basis[j], basis[j + 1], 1, shift, group_lay, half)
        gram(2 * j + 2, basis[j + 1], basis[j + 1], shift, shift, group_lay, half)

    def wave(w):
        relay(w)
        arrived(w)

        @pl.when(w + AHEAD < CHUNKS)
        def _():
            first(w + AHEAD)

        pl.when(w == 1)(diag_arrived)
        for j in range(ITERS):
            @pl.when(w >= j + 1)
            def _():
                apply(j, w - j - 1)

    def back(j, low, high, layer):
        def run(ch, carry):
            back_copy(j, ch, layer).start()
            return carry

        lax.fori_loop(low, high, run, 0)

    chunks(wave)
    for tail in range(ITERS):
        for j in range(tail, ITERS):
            apply(j, CHUNKS - 1 + tail - j)
        if tail == 0:
            back(1, 0, CHUNKS // 2, 0)
        if tail == 1:
            back(1, CHUNKS // 2, CHUNKS, 0)
            for layer in range(1, lay):
                back(1, 0, CHUNKS, layer)
        grams(tail)

    count = acc.shape[0]
    sums = nt_dot(jnp.ones((8, 128), jnp.float32), acc[...])
    lane_q = lax.broadcasted_iota(jnp.int32, (8, count), 1)
    row_q = lax.broadcasted_iota(jnp.int32, (8, count), 0)
    q = lax.broadcasted_iota(jnp.int32, (count, 128), 0)
    c = lax.broadcasted_iota(jnp.int32, (count, 128), 1)
    pick = (q // (blk * blk) == c // blk) & (q % blk == c % blk)
    kept = jnp.where((lane_q // blk) % blk == row_q, sums, 0.0)
    local = dot(kept, jnp.where(pick, 1.0, 0.0))
    mine[...] = local
    slots1[gy] = local

    def along(n, me, src, slots, send, recv, axis):
        at = (lambda i: (gz, i)) if axis == "gy" else (lambda i: (i, gy))
        for off in range(1, n):
            to = (me + off) % n
            remote(src, slots.at[me], send.at[to], recv.at[me], at(to)).start()
        if axis == "gz":
            for layer in range(lay):
                back(2, 0, CHUNKS, layer)
        for off in range(1, n):
            frm = (me + off) % n
            remote(src, slots.at[frm], send.at[frm], recv.at[frm], at(frm)).wait()
        total = slots[0]
        for i in range(1, n):
            total = total + slots[i]
        return total

    summed = along(n_y, gy, mine, slots1, g1_s, g1_r, "gy")
    part[...] = summed
    slots2[gz] = summed
    moments = along(n_z, gz, part, slots2, g2_s, g2_r, "gz")

    lane = lax.broadcasted_iota(jnp.int32, (8, 128), 1)
    keep = lambda x, low, high: jnp.where((lane >= low) & (lane < high), x, 0.0)
    left_by = lambda x, n: x if n == 0 else pltpu.roll(x, 128 - n, 1)
    order = (ITERS + 1) * blk
    lane32 = lax.broadcasted_iota(jnp.int32, (order, 128), 1)
    row32 = lax.broadcasted_iota(jnp.int32, (order, 128), 0)
    full = jnp.concatenate(
        [keep(left_by(moments, blk * i), 0, order) for i in range(ITERS + 1)], axis=0
    )
    full = full + jnp.where(lane32 == row32 + order, 1.0, 0.0)
    inv = 1.0 / SCALE
    second = (
        (inv * inv) * left_by(moments, 2 * blk)
        + (2.0 * CENTRE * inv) * left_by(moments, blk)
        + (CENTRE * CENTRE) * moments
    )
    target = inv * left_by(moments, blk) + CENTRE * moments
    small = ITERS * blk
    normal = jnp.concatenate(
        [
            keep(left_by(second, blk * i), 0, small)
            + keep(pltpu.roll(target, small - blk * i, 1) if i < ITERS else target, small, order)
            for i in range(ITERS)
        ],
        axis=0,
    )
    rows_small = lax.broadcasted_iota(jnp.int32, (small, 1), 0)
    rows_full = lax.broadcasted_iota(jnp.int32, (order, 1), 0)
    for k in range(order):
        if k < small:
            row = normal[k:k + 1] / normal[k:k + 1, k:k + 1]
            column = jnp.where(rows_small == k, 0.0, normal[:, k:k + 1])
            normal = jnp.where(rows_small == k, row, normal - column * row)
        row = full[k:k + 1] / full[k:k + 1, k:k + 1]
        column = jnp.where(rows_full <= k, 0.0, full[:, k:k + 1])
        full = full - column * row
    pivots = jnp.sum(jnp.where(lane32 == row32, full, 0.0), axis=1, keepdims=True)
    full = full / jnp.sqrt(pivots)
    upper = jnp.where((lane32 < order) & (lane32 >= row32), full, 0.0)
    lower_inv = left_by(full, order)
    lower_inv = jnp.where(lane32 < small, lower_inv, 0.0)[:small]
    hess = inv * nt_dot(pltpu.roll(lower_inv, blk, 1), upper)
    eye = lax.broadcasted_iota(jnp.int32, (small, order), 0) == lax.broadcasted_iota(
        jnp.int32, (small, order), 1
    )
    row_b = lax.broadcasted_iota(jnp.int32, (small, order), 0) // blk
    col_b = lax.broadcasted_iota(jnp.int32, (small, order), 1) // blk
    hess = hess + jnp.where(eye, CENTRE, 0.0)
    hess_ref[...] = jnp.where(col_b <= row_b + 1, hess, 0.0)

    for k in range(small):
        for u in range(blk):
            splat[k * blk + u] = jnp.broadcast_to(
                normal[k:k + 1, small + u:small + u + 1], (8, 128)
            )

    def combine(dst, layers, row_start, height, sources):
        tiles = height // 8

        def run(i, carry):
            layer, t = layers[0] + i // tiles, i % tiles
            at = pl.multiple_of(row_start + t * 8, 8)
            for lane_at in range(lanes):
                cols = pl.ds(lane_at * 128, 128)
                vals = []
                for ref, l_at, base in sources:
                    first_row = pl.multiple_of(base + t * 8, 8)
                    vals += [ref[v, l_at + layer, pl.ds(first_row, 8), cols] for v in range(blk)]
                for u in range(blk):
                    total = splat[u] * vals[0]
                    for k in range(1, small):
                        total = total + splat[k * blk + u] * vals[k]
                    dst[u, layer, pl.ds(at, 8), cols] = total
            return carry

        lax.fori_loop(0, (layers[1] - layers[0]) * tiles, run, 0)

    for layer in range(lay):
        combine(held, (layer, layer + 1), 0, late, [(k, 1 + theirs_at, early) for k in basis[:ITERS]])
        late_copy(layer).start()
    combine(
        out_ref, (0, lay), hs, half, ((r_ref, 0, hs), (k1, 1 + mine_at, 0), (k2, 1 + mine_at, 0))
    )

    def back_wait(ch):
        for j in (1, 2):
            for layer in range(lay):
                back_copy(j, ch, layer).wait()

    chunks(back_wait)
    combine(out_ref, (0, lay), os, early, ((r_ref, 0, os), (ret1, 0, 0), (ret2, 0, 0)))
    for layer in range(lay):
        late_copy(layer).wait_send()
        remote(
            held.at[:, pl.ds(layer, 1)],
            out_ref.at[:, pl.ds(layer, 1), pl.ds(pl.multiple_of(os + early, 8), late)],
            l_s.at[layer], l_r.at[layer], (partner, gy),
        ).wait_recv()

    def drain(ch):
        for which in (0, 1):
            exchange(which, ch).wait_send()
        for j in range(ITERS):
            @pl.when(below)
            def _():
                z_copy(j, ch, 0).wait_send()

            @pl.when(above)
            def _():
                z_copy(j, ch, 1).wait_send()

            @pl.when(before)
            def _():
                y_copy(j, ch, 0).wait_send()

            @pl.when(after)
            def _():
                y_copy(j, ch, 1).wait_send()

    chunks(drain)
    diag_copy.wait_send()


def body(right_side, diagonal):
    blk, lay, rows, nx = right_side.shape
    half, group_lay = rows // 2, 2 * lay
    early = half * EARLY // 32 * 8
    n_z, n_y = lax.axis_size("gz"), lax.axis_size("gy")
    vmem = lambda *shape: pltpu.VMEM(shape, jnp.float32)
    dma = lambda *shape: pltpu.SemaphoreType.DMA(shape)
    small, order = ITERS * blk, (ITERS + 1) * blk
    return pl.pallas_call(
        kernel,
        out_shape=(
            jax.ShapeDtypeStruct(right_side.shape, jnp.float32),
            jax.ShapeDtypeStruct((small, order), jnp.float32),
        ),
        in_specs=[pl.BlockSpec(memory_space=pltpu.VMEM)] * 2,
        out_specs=(pl.BlockSpec(memory_space=pltpu.VMEM),) * 2,
        scratch_shapes=[
            vmem(blk, group_lay + 2, half, nx),
            vmem(blk, group_lay + 2, half, nx),
            vmem(blk, group_lay + 2, half, nx),
            vmem(blk, group_lay, half, nx),
            vmem(group_lay, half, nx),
            vmem(blk, lay, early, nx),
            vmem(blk, lay, early, nx),
            vmem(blk, lay, half - early, nx),
            vmem(ITERS, 2, blk, group_lay, nx),
            vmem(ITERS, 2, blk, group_lay, nx),
            vmem(8 * blk * blk, 128),
            vmem(8, 128),
            vmem(n_y, 8, 128),
            vmem(8, 128),
            vmem(n_z, 8, 128),
            vmem(small * blk, 8, 128),
            dma(2, CHUNKS), dma(2, CHUNKS),
            pltpu.SemaphoreType.DMA, pltpu.SemaphoreType.DMA,
            dma(ITERS, 2, CHUNKS), dma(ITERS, 2, CHUNKS),
            dma(ITERS, 2, CHUNKS), dma(ITERS, 2, CHUNKS),
            dma(2, lay, CHUNKS), dma(2, lay, CHUNKS), dma(lay), dma(lay),
            dma(n_y), dma(n_y), dma(n_z), dma(n_z),
        ],
        compiler_params=pltpu.CompilerParams(
            collective_id=0, has_side_effects=True, vmem_limit_bytes=60 * 1024 * 1024
        ),
        name="gmres",
    )(right_side, diagonal)


def solution(mesh):
    in_specs = (P(None, "gz", "gy", None), P("gz", "gy", None))
    out_specs = (P(None, "gz", "gy", None), P())
    return jax.shard_map(body, mesh=mesh, in_specs=in_specs, out_specs=out_specs, check_vma=False)
```
